128 devices in a mesh: obs: 4 (over z), face: 32 (over x, y, core).
Axes of the slice: x: 4, y: 4, z: 4, core: 2. Of those that a mesh axis runs over, the one named last changes fastest.
Arguments:
- density: float32 [34, 32768], P(None, ('obs', 'face')), may hold values from 0.6 to 1.4
- velocity: float32 [3, 34, 32768], P(None, None, ('obs', 'face')), may hold values from -6 to 6
- pressure: float32 [34, 32768], P(None, ('obs', 'face')), may hold values from -6 to 6
- normal: float32 [3, 32768], P(None, ('obs', 'face')), may hold values from -1 to 1, as said below
- direction: float32 [128, 32, 3], P(('obs', 'face')), may hold values from -1 to 1, as said below
- weights: bfloat16 [128, 32, 768, 256], P(('obs', 'face')), may hold values from -0.21875 to 0.21875
- bin_index: int32 [128, 32], P(('obs', 'face')), may hold values from 0 to 31, as said below
- group_index: int32 [128, 32], P(('obs', 'face')), may hold values from 0 to 3
- item_count: int32 [128], P(('obs', 'face')), may hold values from 16 to 32, as said below
Outputs:
- signal: float32 [1024, 1024], P('face', 'obs')
The draws below stay inside these ranges and needn't reach their ends.
Inputs may be any that keep to these rules, and one draw needn't show every extreme that they name: `bin_index`: no time block is named more than 2 times in one device's list; in every draw some device names a block 2 times among its live entries. `item_count`: some device has all 32 entries live. Each face's normal has unit length. Each entry's direction has unit length.
All inputs are finite; a program needn't handle non-finite values.
Results may differ from the reference program's by a relative error of at most 0.0029.
Values sent between devices are 32-bit elements; how exact they have to be, the bound alone decides.
No kernel may reach another device: no remote copies, remote signals or barrier semaphores. Data moves between devices by JAX's collectives and lax.ppermute only.
A program may use at most 64 MiB of HBM per device.

```python
import math
import jax
import jax.numpy as jnp
from jax import lax

FACE_DEV = 256
OBS_GROUP = 256
WINDOW_STEPS = 32
SLOT_CAP = 2
LIST_LEN = 32
TOTAL_FACES = 32768
OBSERVERS = 1024
SAMPLES = 1024
DEVICES = 128


def unit_vectors(key, count):
    first, second = jax.random.split(key)
    height = jax.random.uniform(first, (count,), jnp.float32, -1.0, 1.0)
    azimuth = jax.random.uniform(second, (count,), jnp.float32, -math.pi, math.pi)
    radius = jnp.sqrt(jnp.maximum(1.0 - height * height, 0.0))
    return (radius * jnp.cos(azimuth), radius * jnp.sin(azimuth), height)


def draw_normal(key, part):
    east, north, upward = unit_vectors(jax.random.fold_in(key, 11), TOTAL_FACES)
    return jnp.stack([east, north, upward], axis=0).astype(jnp.float32)


def draw_direction(key, part):
    devices = TOTAL_FACES // FACE_DEV
    east, north, upward = unit_vectors(jax.random.fold_in(key, 12), devices * LIST_LEN)
    return jnp.stack([east, north, upward], axis=-1).reshape(devices, LIST_LEN, 3).astype(jnp.float32)


def draw_bin_index(key, part):
    devices = TOTAL_FACES // FACE_DEV
    n_blocks = SAMPLES // WINDOW_STEPS

    def one_row(row_key):
        order_key, block_key = jax.random.split(row_key)
        order = jax.random.permutation(order_key, LIST_LEN)
        blocks = jax.random.permutation(block_key, n_blocks)
        return blocks[order // SLOT_CAP].astype(jnp.int32)
    return jax.vmap(one_row)(jax.random.split(jax.random.fold_in(key, 13), devices))


def draw_item_count(key, part):
    devices = TOTAL_FACES // FACE_DEV
    first, second, third = jax.random.split(jax.random.fold_in(key, 14), 3)
    base = jax.random.randint(first, (devices,), LIST_LEN // 2, LIST_LEN + 1)
    full = jax.random.randint(second, (devices,), 0, 8) == 0
    chosen = jax.random.randint(third, (), 0, devices)
    forced = jnp.arange(devices) == chosen
    return jnp.where(full | forced, LIST_LEN, jnp.minimum(base, LIST_LEN)).astype(jnp.int32)


def plant(array, rng, low, top_value):
    longest = array.shape.index(max(array.shape))
    spots = []
    for shift in (0, 1):
        where = [jax.random.randint(jax.random.fold_in(rng, axis), (), 0, length) for axis, length in enumerate(array.shape)]
        where[longest] = (where[longest] + shift) % array.shape[longest]
        spots.append(tuple(where))
    return array.at[spots[0]].set(low).at[spots[1]].set(top_value)


def steps_of(key, shape, cuts, smallest, high):
    level, own = 1.0, jax.random.fold_in(key, 6)
    for axis_at, parts in cuts:
        draws = jnp.exp(jax.random.uniform(jax.random.fold_in(own, axis_at), (parts,), jnp.float32, smallest / len(cuts), high / len(cuts)))
        level = level * jnp.repeat(draws, shape[axis_at] // parts).reshape([-1 if axis == axis_at else 1 for axis in range(len(shape))])
    return level


def bell_draw(own_key, extent, width, bound, cuts=(), kind=jnp.bfloat16):
    loudness = steps_of(own_key, extent, cuts, -0.22, 0.18) if cuts else 1.0
    result = jax.random.normal(own_key, extent, jnp.float32) * width * loudness
    return jnp.minimum(jnp.maximum(result, -bound), bound).astype(kind)


def setup_inputs(seed: int = 0) -> dict:
    splits = jax.random.split(jax.random.key(seed), 10)
    density = jnp.clip(0.6 + 0.79999995 * jax.random.uniform(splits[0], (WINDOW_STEPS + 2, TOTAL_FACES), jnp.float32) ** steps_of(splits[0], (WINDOW_STEPS + 2, TOTAL_FACES), ((1, 128),), -0.2, 0.2), 0.6, 1.4)
    velocity = bell_draw(splits[1], (3, WINDOW_STEPS + 2, TOTAL_FACES), 1.0, 6.0, ((2, 128),), jnp.float32)
    pressure = bell_draw(splits[2], (WINDOW_STEPS + 2, TOTAL_FACES), 1.0, 6.0, ((1, 128),), jnp.float32)
    normal = draw_normal(jax.random.fold_in(splits[9], 71), 0)
    direction = draw_direction(jax.random.fold_in(splits[9], 71), 0)
    weights = bell_draw(splits[5], (DEVICES, LIST_LEN, 3 * FACE_DEV, OBS_GROUP), (3 * FACE_DEV) ** -0.5, 0.21875, ((0, 128),))
    bin_index = draw_bin_index(jax.random.fold_in(splits[9], 71), 0)
    group_index = plant(jax.random.randint(splits[7], (DEVICES, LIST_LEN), 0, OBSERVERS // OBS_GROUP), jax.random.fold_in(splits[7], 1), 0, (OBSERVERS // OBS_GROUP) - 1).astype(jnp.int32)
    item_count = draw_item_count(jax.random.fold_in(splits[9], 71), 0)
    return dict(density=density, velocity=velocity, pressure=pressure, normal=normal, direction=direction, weights=weights, bin_index=bin_index, group_index=group_index, item_count=item_count)


def face_terms(dens, veloc, press, norms):
    normal_speed = veloc[0] * norms[0][None] + veloc[1] * norms[1][None] + veloc[2] * norms[2][None]
    flux = dens * normal_speed
    load_first = press * norms[0][None] + dens * veloc[0] * normal_speed
    load_second = press * norms[1][None] + dens * veloc[1] * normal_speed
    load_third = press * norms[2][None] + dens * veloc[2] * normal_speed
    thick = 0.5 * (flux[2:] - flux[:-2])
    return thick, load_first, load_second, load_third


def item_source(thick, load_first, load_second, load_third, heading):
    radial = heading[0] * load_first + heading[1] * load_second + heading[2] * load_third
    rate = 0.5 * (radial[2:] - radial[:-2])
    return jnp.concatenate([thick, rate, radial[1:-1]], axis=1).astype(jnp.bfloat16)


def reference(density, velocity, pressure, normal, direction, weights, bin_index, group_index, item_count):
    n_devices = weights.shape[0]
    per_device = density.shape[1] // n_devices
    rows = density.shape[0]
    dens_dev = density.reshape(rows, n_devices, per_device).transpose(1, 0, 2)
    press_dev = pressure.reshape(rows, n_devices, per_device).transpose(1, 0, 2)
    veloc_dev = velocity.reshape(3, rows, n_devices, per_device).transpose(2, 0, 1, 3)
    norms_dev = normal.reshape(3, n_devices, per_device).transpose(1, 0, 2)
    n_blocks = SAMPLES // WINDOW_STEPS
    n_groups = OBSERVERS // OBS_GROUP
    start = jnp.zeros((n_blocks, n_groups, WINDOW_STEPS, OBS_GROUP), jnp.float32)

    def device_step(signal, inputs):
        dens, veloc, press, norms, headings, matrices, blocks_of, groups_of, live_count = inputs
        thick, load_first, load_second, load_third = face_terms(dens, veloc, press, norms)
        for listed in range(LIST_LEN):
            source = item_source(thick, load_first, load_second, load_third, headings[listed])
            block = jnp.dot(source, matrices[listed], preferred_element_type=jnp.float32)
            switch = (listed < live_count).astype(jnp.float32)
            signal = signal.at[blocks_of[listed], groups_of[listed]].add(block * switch)
        return signal, None

    signal, _ = lax.scan(device_step, start, (dens_dev, veloc_dev, press_dev, norms_dev, direction, weights, bin_index, group_index, item_count))
    return signal.transpose(0, 2, 1, 3).reshape(SAMPLES, OBSERVERS)
```

```python
import jax
import jax.numpy as jnp
from jax import lax
from jax.experimental import pallas as pl
from jax.experimental.pallas import tpu as pltpu
from jax.sharding import PartitionSpec as P

SLOT_CAP = 2
DEPTH = 8
UNROLL = 2


def item_kernel(
    bins, groups, count, headings, dens, veloc, press, norms, matrices,
    outgoing, labels, ring, linear, thick, slots, named, sems,
):
    list_total, _, width = matrices.shape[1:]
    live = count[0]

    def fetch(listed):
        spot = lax.rem(listed, DEPTH)
        return pltpu.make_async_copy(matrices.at[0, listed], ring.at[spot], sems.at[spot])

    for listed in range(DEPTH):
        @pl.when(listed < live)
        def _():
            fetch(listed).start()

    faces = dens.shape[1]
    face_terms(dens, veloc, press, norms, linear, thick)
    outgoing[...] = jnp.zeros_like(outgoing)

    def clear(block, carry):
        named[block] = 0
        labels[block * SLOT_CAP] = 0.0
        labels[block * SLOT_CAP + 1] = 0.0
        return carry

    lax.fori_loop(0, named.shape[0], clear, 0)

    def place(listed, carry):
        block = bins[0, listed]
        target = block * SLOT_CAP + named[block]
        named[block] = named[block] + 1
        slots[listed] = target
        labels[target] = groups[0, listed].astype(jnp.float32)
        return carry

    lax.fori_loop(0, live, place, 0)

    def step(turn, carry):
        for part in range(UNROLL):
            listed = turn * UNROLL + part

            @pl.when(listed < live)
            def _():
                fetch(listed).wait()

        for part in range(UNROLL):
            listed = turn * UNROLL + part
            valid = listed < live
            known = jnp.where(valid, listed, 0)
            spot = lax.rem(listed, DEPTH)
            mixed = (
                headings[0, 0, known] * linear[0]
                + headings[1, 0, known] * linear[1]
                + headings[2, 0, known] * linear[2]
            ).astype(jnp.bfloat16)
            source = jnp.concatenate([thick[...], mixed], axis=1)
            block = jnp.dot(source, ring[spot], preferred_element_type=jnp.float32)
            target = slots[known]
            outgoing[target] = jnp.where(valid, block, outgoing[target])

        for part in range(UNROLL):
            listed = turn * UNROLL + part + DEPTH

            @pl.when(listed < live)
            def _():
                fetch(listed).start()

        return carry

    lax.fori_loop(0, pl.cdiv(live, UNROLL), step, 0)


def face_terms(dens, veloc, press, norms, linear, thick):
    faces = dens.shape[1]
    across = [norms[axis : axis + 1, :] for axis in range(3)]
    moving = [veloc[axis] for axis in range(3)]
    density = dens[...]
    pressure = press[...]
    normal_speed = moving[0] * across[0] + moving[1] * across[1] + moving[2] * across[2]
    flux = density * normal_speed
    thick[...] = (0.5 * (flux[2:] - flux[:-2])).astype(jnp.bfloat16)
    for axis in range(3):
        load = pressure * across[axis] + density * moving[axis] * normal_speed
        linear[axis, :, :faces] = 0.5 * (load[2:] - load[:-2])
        linear[axis, :, faces:] = load[1:-1]


def local(
    density, velocity, pressure, normal, direction, weights, bin_index, group_index, item_count
):
    n_face = lax.axis_size("face")
    n_obs = lax.axis_size("obs")
    list_total, depth, width = weights.shape[1:]
    steps = density.shape[0] - 2
    faces = density.shape[1]
    headings = direction.transpose(2, 0, 1)
    smem = pl.BlockSpec(memory_space=pltpu.SMEM)
    vmem = pl.BlockSpec(memory_space=pltpu.VMEM)
    outgoing, labels = pl.pallas_call(
        item_kernel,
        out_shape=(
            jax.ShapeDtypeStruct((n_face * SLOT_CAP, steps, width), jnp.float32),
            jax.ShapeDtypeStruct((n_face * SLOT_CAP,), jnp.float32),
        ),
        in_specs=[smem, smem, smem, smem, vmem, vmem, vmem, vmem, pl.BlockSpec(memory_space=pl.ANY)],
        out_specs=(vmem, smem),
        scratch_shapes=[
            pltpu.VMEM((DEPTH, depth, width), jnp.bfloat16),
            pltpu.VMEM((3, steps, 2 * faces), jnp.float32),
            pltpu.VMEM((steps, faces), jnp.bfloat16),
            pltpu.SMEM((list_total,), jnp.int32),
            pltpu.SMEM((n_face,), jnp.int32),
            pltpu.SemaphoreType.DMA((DEPTH,)),
        ],
        name="items",
    )(bin_index, group_index, item_count, headings, density, velocity, pressure, normal, weights)
    arrived, arrived_labels = (
        lax.all_to_all(
            outgoing.reshape(n_face, SLOT_CAP, steps, width),
            "face",
            split_axis=0,
            concat_axis=0,
            tiled=True,
        ),
        lax.all_to_all(
            labels.reshape(n_face, SLOT_CAP), "face", split_axis=0, concat_axis=0, tiled=True
        ),
    )
    selector = (
        arrived_labels.reshape(1, -1) == jnp.arange(n_obs, dtype=jnp.float32)[:, None]
    ).astype(jnp.float32)
    grouped = jnp.dot(
        selector,
        arrived.reshape(n_face * SLOT_CAP, steps * width),
        precision=lax.Precision.HIGHEST,
        preferred_element_type=jnp.float32,
    )
    grouped = grouped.reshape(n_obs, steps, width)
    arrived = lax.all_to_all(grouped, "obs", split_axis=0, concat_axis=0, tiled=True)
    return arrived.sum(axis=0)


def solution(mesh):
    placed = (
        P(None, ("obs", "face")),
        P(None, None, ("obs", "face")),
        P(None, ("obs", "face")),
        P(None, ("obs", "face")),
        P(("obs", "face"), None, None),
        P(("obs", "face"), None, None, None),
        P(("obs", "face"), None),
        P(("obs", "face"), None),
        P(("obs", "face")),
    )
    return jax.shard_map(
        local, mesh=mesh, in_specs=placed, out_specs=P("face", "obs"), check_vma=False
    )
```
